32 devices in a mesh: row: 8 (over y, x, core), col: 4 (over z).
Axes of the slice: x: 2, y: 2, z: 4, core: 2. Of those that a mesh axis runs over, the one named last changes fastest.
Arguments:
- queries: bfloat16 [32768, 768], P(('row', 'col'))
- documents: bfloat16 [1024, 768], P(('row', 'col'))
- counts: int32 [32], P(('row', 'col')), may hold values from 2 to 32, as said below
- positives: int32 [32768], P(('row', 'col')), may hold values from 0 to 1023, as said below
Outputs:
- losses: float32 [32768], P(('row', 'col'))
The draws below stay inside these ranges and needn't reach their ends.
Inputs may be any that keep to these rules, and one draw needn't show every extreme that they name: `counts`: some block has exactly 32 valid slots in every draw. Each names a valid slot: positives[i] % 32 < counts[positives[i] // 32].
All inputs are finite; a program needn't handle non-finite values.
Results may differ from the reference program's by a relative error of at most 0.0003.
Values may be sent and summed in bfloat16 or wider, within the bound.
A program may use at most 128 MiB of HBM per device.

```python
import jax
import jax.numpy as jnp
from jax import lax

D = 768
Q_DEV = 1024
DOC_DEV = 32
QUERIES = 32768
DOCS = 1024
DEVICES = 32


def shared_ints(key):
    counts = jax.random.randint(jax.random.fold_in(key, 11), (DEVICES,), 2, DOC_DEV + 1)
    full = jax.random.randint(jax.random.fold_in(key, 13), (), 0, DEVICES)
    counts = jnp.where(jnp.arange(DEVICES) == full, DOC_DEV, counts).astype(jnp.int32)
    owner = jax.random.randint(jax.random.fold_in(key, 12), (QUERIES,), 0, DEVICES)
    raw = jax.random.randint(jax.random.fold_in(key, 14), (QUERIES,), 0, 1000000)
    slot = raw % counts[owner]
    return (counts, (owner * DOC_DEV + slot).astype(jnp.int32))


def shared_floats(key):
    docs = jax.random.normal(jax.random.fold_in(key, 21), (DOCS, D), jnp.float32)
    quer = jax.random.normal(jax.random.fold_in(key, 22), (QUERIES, D), jnp.float32)
    return (quer, docs)


def draw_queries(key, part):
    return shared_floats(key)[0].astype(jnp.bfloat16)


def draw_documents(key, part):
    return shared_floats(key)[1].astype(jnp.bfloat16)


def draw_counts(key, part):
    return shared_ints(key)[0]


def draw_positives(key, part):
    return shared_ints(key)[1]


def setup_inputs(seed: int = 0) -> dict:
    splits = jax.random.split(jax.random.key(seed), 5)
    return {
        "queries": draw_queries(jax.random.fold_in(splits[4], 71), 0),
        "documents": draw_documents(jax.random.fold_in(splits[4], 71), 0),
        "counts": draw_counts(jax.random.fold_in(splits[4], 71), 0),
        "positives": draw_positives(jax.random.fold_in(splits[4], 71), 0),
    }


def reference(queries, documents, counts, positives):
    slot = jnp.arange(DOCS, dtype=jnp.int32)
    valid = (slot % DOC_DEV) < counts[slot // DOC_DEV]
    total = jnp.sum(counts.astype(jnp.float32))
    scale = D ** -0.5
    query_blocks = queries.reshape(DEVICES, Q_DEV, D)
    pos_blocks = positives.reshape(DEVICES, Q_DEV)

    def one_block(pair):
        block, wanted = pair
        scores = jnp.dot(block, documents.T, preferred_element_type=jnp.float32) * scale
        masked = jnp.where(valid[None, :], scores, -1e30)
        top = jnp.max(masked, axis=1)
        lse = top + jnp.log(jnp.sum(jnp.exp(masked - top[:, None]), axis=1))
        picked = jnp.take_along_axis(scores, wanted[:, None].astype(jnp.int32), axis=1)[:, 0]
        return lse - picked - jnp.log(total)

    return lax.map(one_block, (query_blocks, pos_blocks)).reshape(QUERIES)
```

```python
import functools
import math

import jax
import jax.numpy as jnp
from jax import lax
from jax.experimental import pallas as pl
from jax.experimental.pallas import tpu as pltpu
from jax.sharding import PartitionSpec as P

MESH = pl.DeviceIdType.MESH
very_low = -1e30
LOG2E = math.log2(math.e)
GRANT = 55232 * 1024


def kernel(rows, cols, counts_hbm, docs_hbm, quer_hbm, pos_hbm, out_ref,
           counts_ref, pos_ref, block, buf, quer, run_max, run_sum, run_pos, run_cnt,
           counts_sem, pos_sem, own_sem, quer_sem, send_sem, recv_sem):
    slots, feat = block.shape
    nq = quer.shape[0]
    scale = feat ** -0.5
    k2 = scale * LOG2E
    direct, along = (0, cols - 1), tuple(range(1, cols - 1))
    pairs = rows // 2
    nb = 2 if pairs % 2 == 0 else 1
    na = pairs // nb
    r, c = lax.axis_index("row"), lax.axis_index("col")
    core = lax.rem(r, 2)
    a, b = lax.div(r, 2 * nb), lax.rem(lax.div(r, 2), nb)

    def row_at(i, j):
        return (lax.rem(a + i, na) * nb + lax.rem(b + j, nb)) * 2 + core

    def col_at(k):
        if cols & (cols - 1):
            return lax.rem(c + k, cols)
        bits = [1 << n for n in range(cols.bit_length()) if k >> n & 1]
        return c + sum(bit * (1 - 2 * lax.rem(lax.div(c, bit), 2)) for bit in bits)

    def col_to(k):
        if cols & (cols - 1):
            return lax.rem(c + cols - k, cols)
        return col_at(k)

    mate = r + 1 - 2 * core

    partners = [(r, col_at(k)) for k in range(1, cols)]
    partners += [(row_at(i, 0), c) for i in range(1, na)]
    partners += [(row_at(0, j), c) for j in range(1, nb)]
    partners += [(row_at(i, j), c) for i in range(1, na) for j in range(1, nb) if direct]
    partners += [(mate, c)]
    barrier = pltpu.get_barrier_semaphore()
    for who in partners:
        pl.semaphore_signal(barrier, inc=1, device_id=who, device_id_type=MESH)

    counts_copy = pltpu.make_async_copy(counts_hbm, counts_ref, counts_sem)
    counts_copy.start()
    own_copy = pltpu.make_async_copy(docs_hbm, block, own_sem)
    own_copy.start()
    quer_copy = pltpu.make_async_copy(quer_hbm, quer, quer_sem)
    quer_copy.start()
    pos_copy = pltpu.make_async_copy(pos_hbm, pos_ref, pos_sem)
    pos_copy.start()

    own_copy.wait()
    counts_copy.wait()
    slot = lax.broadcasted_iota(jnp.int32, (slots, feat), 0)
    docs = block[...].astype(jnp.float32)
    docs = jnp.where(slot < counts_ref[0], docs, jnp.nan).astype(jnp.bfloat16)
    buf[r, c] = docs
    run_max[...] = jnp.full(run_max.shape, very_low, jnp.float32)
    run_sum[...] = jnp.zeros(run_sum.shape, jnp.float32)
    run_pos[...] = jnp.zeros(run_pos.shape, jnp.float32)
    run_cnt[...] = jnp.zeros(run_cnt.shape, jnp.float32)
    pl.semaphore_wait(barrier, len(partners))

    sent = []

    def copy_of(src_row, src_col, who, n):
        return pltpu.make_async_remote_copy(
            src_ref=buf.at[src_row, src_col],
            dst_ref=buf.at[src_row, src_col],
            send_sem=send_sem.at[n],
            recv_sem=recv_sem.at[src_row, src_col],
            device_id=who,
            device_id_type=MESH,
        )

    def send(src_row, src_col, who):
        copy = copy_of(src_row, src_col, who, len(sent))
        copy.start()
        sent.append(copy)

    def arrive(src_row, src_col):
        copy_of(src_row, src_col, (mate, c), 0).wait_recv()

    def line(k):
        z = col_at(k)
        if k:
            arrive(r, z)
        for i in range(1, na):
            send(r, z, (row_at(i, 0), c))
        for j in range(1, nb):
            send(r, z, (row_at(0, j), c))
        if k in direct:
            for i in range(1, na):
                for j in range(1, nb):
                    send(r, z, (row_at(i, j), c))
        send(r, z, (mate, c))

    def plane(k):
        z = col_at(k)
        for i in range(1, na):
            arrive(row_at(i, 0), z)
        for j in range(1, nb):
            arrive(row_at(0, j), z)
        for i in range(1, 1 if k in direct + along else na):
            for j in range(1, nb):
                src = row_at(i * (1 - core), j * core)
                dst = row_at(i * core, j * (1 - core))
                send(src, z, (dst, c))
        for i in range(1, na):
            send(row_at(i, 0), z, (mate, c))
        for j in range(1, nb):
            send(row_at(0, j), z, (mate, c))

    def corner(k):
        z = col_at(k)
        for i in range(1, na):
            for j in range(1, nb):
                arrive(row_at(i, j), z)
                for n in along if k == 0 else ():
                    send(row_at(i, j), z, (r, col_to(n)))
                send(row_at(i, j), z, (mate, c))

    group = 2 * cols * slots
    piece_cols = min(cols, max(1, 128 // slots))
    tile = 256 if nq % 256 == 0 else nq

    def compute(i, j):
        first = row_at(i, j) - core
        other = row_at(i, j) + 1 - 2 * core
        for k in range(cols):
            arrive(other, col_at(k))

        def piece(n):
            base_col = n * piece_cols
            height = 2 * piece_cols * slots
            d = buf[pl.ds(first, 2), pl.ds(base_col, piece_cols)]
            d = d.reshape(height, feat)
            head = d[:, :128].astype(jnp.float32)
            good = head == head
            run_cnt[...] += jnp.sum(
                jnp.where(good, 1.0, 0.0).reshape(height // 8, 8, 128), axis=0)
            good = jnp.concatenate([good] * (tile // 128), axis=1)
            row_id = lax.broadcasted_iota(jnp.int32, (2, piece_cols * slots, tile), 1)
            half = lax.broadcasted_iota(jnp.int32, (2, piece_cols * slots, tile), 0)
            index = ((first + half) * cols + base_col) * slots + row_id
            index = index.reshape(height, tile)
            for t in range(nq // tile):
                at = pl.ds(t * tile, tile)
                s = lax.dot_general(d, quer[at, :], (((1,), (1,)), ((), ())),
                                    preferred_element_type=jnp.float32)
                hit = jnp.where(index == pos_ref[:, at], s, 0.0)
                run_pos[:, at] += jnp.sum(hit.reshape(height // 8, 8, tile), axis=0)
                s = jnp.where(good, s, very_low).reshape(height // 8, 8, tile)
                old = run_max[:, at]
                new = jnp.maximum(old, jnp.max(s, axis=0))
                e = jnp.exp2((s - new[None]) * k2)
                run_sum[:, at] = (run_sum[:, at] * jnp.exp2((old - new) * k2)
                                  + jnp.sum(e, axis=0))
                run_max[:, at] = new

        if cols == piece_cols:
            piece(0)
        else:
            pl.loop(0, cols // piece_cols)(piece)

    near = [(i, 0) for i in range(1, na)] + [(0, j) for j in range(1, nb)]
    far = [(i, j) for i in range(1, na) for j in range(1, nb)]
    for k in range(1, cols):
        send(r, c, (r, col_to(k)))
    line(0)
    for k in range(1, cols):
        line(k)
        if k == 1:
            plane(0)
            corner(0)
    quer_copy.wait()
    pos_copy.wait()
    for k in range(1, cols - 1):
        plane(k)
        corner(k)
    compute(0, 0)
    if cols > 1:
        plane(cols - 1)
        corner(cols - 1)
    for i, j in near + far:
        compute(i, j)

    top = jnp.max(run_max[...], axis=0, keepdims=True)
    total = jnp.sum(run_sum[...] * jnp.exp2((run_max[...] - top) * k2), axis=0, keepdims=True)
    picked = jnp.sum(run_pos[...], axis=0, keepdims=True)
    docs_total = jnp.log(jnp.sum(run_cnt[...], axis=0, keepdims=True))
    docs_total = jnp.concatenate([docs_total] * (nq // 128), axis=1)
    out_ref[...] = (top - picked) * scale + jnp.log(total) - docs_total
    for copy in sent:
        copy.wait_send()


def solution(mesh):
    rows, cols = mesh.shape["row"], mesh.shape["col"]

    def shards(queries, documents, counts, positives):
        nq, feat = queries.shape
        slots = documents.shape[0]
        blocks = rows * cols
        out = pl.pallas_call(
            functools.partial(kernel, rows, cols),
            out_shape=jax.ShapeDtypeStruct((1, nq), jnp.float32),
            in_specs=[
                pl.BlockSpec(memory_space=pl.ANY),
                pl.BlockSpec(memory_space=pl.ANY),
                pl.BlockSpec(memory_space=pl.ANY),
                pl.BlockSpec(memory_space=pl.ANY),
            ],
            out_specs=pl.BlockSpec(memory_space=pltpu.VMEM),
            scratch_shapes=[
                pltpu.SMEM((1,), jnp.int32),
                pltpu.VMEM((1, nq), jnp.int32),
                pltpu.VMEM((slots, feat), jnp.bfloat16),
                pltpu.VMEM((rows, cols, slots, feat), jnp.bfloat16),
                pltpu.VMEM((nq, feat), jnp.bfloat16),
                pltpu.VMEM((8, nq), jnp.float32),
                pltpu.VMEM((8, nq), jnp.float32),
                pltpu.VMEM((8, nq), jnp.float32),
                pltpu.VMEM((8, 128), jnp.float32),
                pltpu.SemaphoreType.DMA,
                pltpu.SemaphoreType.DMA,
                pltpu.SemaphoreType.DMA,
                pltpu.SemaphoreType.DMA,
                pltpu.SemaphoreType.DMA((blocks - 1,)),
                pltpu.SemaphoreType.DMA((rows, cols)),
            ],
            compiler_params=pltpu.CompilerParams(
                collective_id=0, has_side_effects=True,
                vmem_limit_bytes=GRANT - 4 * nq,
            ),
        )(counts, documents, queries, positives.reshape(1, nq))
        return out.reshape(nq)

    return jax.shard_map(
        shards,
        mesh=mesh,
        in_specs=(
            P(("row", "col"), None),
            P(("row", "col"), None),
            P(("row", "col")),
            P(("row", "col")),
        ),
        out_specs=P(("row", "col")),
        check_vma=False,
    )
```
